128 devices in a mesh: branch: 4 (over z_lo, core), shard: 32 (over y, x, z_hi).
Axes of the slice: x: 4, y: 4, z: 4 (z_hi: 2, z_lo: 2; z = z_hi * 2 + z_lo), core: 2. Of those that a mesh axis runs over, the one named last changes fastest.
Arguments:
- attention_weights: bfloat16 [4, 2, 4096, 4096], P('branch', None, None, 'shard'), may hold values from -1.25 to 1.25
- ffn_weights: bfloat16 [4, 3, 4096, 11008], P('branch', None, 'shard'), may hold values from -0.3125 to 0.3125
- tokens: bfloat16 [2048, 4096], P(('branch', 'shard')), may hold values from -6 to 6
- routes: int32 [2048, 2], P(('branch', 'shard')), may hold values from 0 to 3, all different within a row; in each aligned block of 16 rows (0 to 15, 16 to 31, ...) at most 12 rows name the same one
- router: bfloat16 [4096, 4], replicated, may hold values from -0.09375 to 0.09375
Outputs:
- merged_attention: bfloat16 [2, 4096, 4096], P(None, 'branch', 'shard')
- expert_weights: bfloat16 [4, 3, 4096, 11008], P('branch', None, None, 'shard')
- mixed_output: bfloat16 [2048, 4096], P(('branch', 'shard'))
The draws below stay inside these ranges and needn't reach their ends.
Inputs may be any that keep to these rules, and one draw needn't show every extreme that they name: `routes`: the 2 experts of a row differ. In each aligned block of 16 rows (the rows of one device) no expert is named by more than 12 rows, and in some blocks one expert is named by exactly 12 rows.
All inputs are finite; a program needn't handle non-finite values.
Results may differ from the reference program's by a relative error of at most 0.018.
Values may be sent and summed in bfloat16 or wider, within the bound.
A program may use at most 192 MiB of HBM per device.

```python
import math
import jax
import jax.numpy as jnp
import numpy as np
from jax import lax

D = 4096
FF = 11008
ATT_MATS = 2
TOP = 2
TOK_DEV = 16
CAP = 12
EXPERTS = 4
TOKENS = 2048
N_BRANCH = 4
N_SHARD = 32
DEVICES = 128


def block_scale(key, dims, pieces, low, top_value):
    level, own = 1.0, jax.random.fold_in(key, 6)
    for dim, shards_of in pieces:
        steps = jnp.exp(jax.random.uniform(jax.random.fold_in(own, dim), (shards_of,), jnp.float32, low / len(pieces), top_value / len(pieces)))
        level = level * jnp.repeat(steps, dims[dim] // shards_of).reshape([-1 if axis == dim else 1 for axis in range(len(dims))])
    return level


def routed_block(own_key, own, number, rows, count, top, most, lean):
    order = jax.random.permutation(own_key, count)
    crowded, common = portions_of(count, rows * top, most, lean, True), portions_of(count, rows * top, most, lean, False)
    places = jnp.arange(count)

    def named(sizes, offset_by):
        used = int((sizes > 0).sum())
        fixed = max(1, used // 4)
        passed = fixed + (places - fixed + offset_by * (used - fixed)) % max(1, count - fixed)
        return jnp.zeros((count,), jnp.int32).at[order[jnp.where(places < fixed, places, passed)]].set(jnp.asarray(sizes, jnp.int32))

    sizes = jnp.where(number % 4 == 0, named(crowded, number // 4), named(common, number - number // 4 - 1))
    mixed = jax.random.permutation(jax.random.fold_in(own, 3), count)
    source_of, sink = mixed[0:count // 2 * 2:2], mixed[1:count // 2 * 2:2]
    room = jnp.minimum(sizes[source_of] - 1, most - sizes[sink]) // 2
    room = jnp.where((source_of == order[0]) | (sink == order[0]) | (sizes[sink] == 0), 0, jnp.maximum(room, 0))
    passed = jax.random.randint(jax.random.fold_in(own, 4), (count // 2,), 0, 1 << 20) % (room + 1)
    sizes = sizes.at[source_of].add(-passed).at[sink].add(passed)
    labels = jnp.searchsorted(jnp.cumsum(sizes), jnp.arange(rows * top), side="right").astype(jnp.int32)
    table = labels.reshape(top, rows).T
    table = table[jax.random.permutation(jax.random.fold_in(own, 1), rows)]
    offset_by = jax.random.randint(jax.random.fold_in(own, 2), (rows, 1), 0, top)
    return jnp.take_along_axis(table, (jnp.arange(top)[None, :] + offset_by) % top, axis=1)


def portions_of(amount, total, most, slope, full):
    portions = [(1 << 20) // math.isqrt(rank ** slope) + 1 for rank in range(1, amount + 1)]
    largest = most if full else min(most, max(-(-total // amount), total * portions[0] // sum(portions)))
    least = 1 if total - largest >= amount - 1 else 0
    given, surplus = [largest] + [least] * (amount - 1), total - largest - least * (amount - 1)
    while surplus > 0:
        free = [i for i in range(1, amount) if given[i] < largest] or [i for i in range(1, amount) if given[i] < most]
        whole, budget = sum([portions[i] for i in free]), surplus
        for i in free:
            more = min(most - given[i], max(1, budget * portions[i] // whole), surplus)
            given[i] = given[i] + more
            surplus = surplus - more
    return np.array(given)


def scatter_about(key, shape, scale, most, split=(), kind=jnp.bfloat16):
    array = jax.random.normal(key, shape, jnp.float32) * scale
    if len(split) > 0:
        array = block_scale(key, shape, split, -0.22, 0.18) * array
    return jnp.clip(array, min=-most, max=most).astype(kind)


def setup_inputs(seed: int = 0) -> dict:
    splits = jax.random.split(jax.random.key(seed), 6)
    attention_weights = scatter_about(splits[0], (EXPERTS, ATT_MATS, D, D), 0.08, 1.25, ((0, 4), (3, 32)))
    ffn_weights = scatter_about(splits[1], (EXPERTS, 3, D, FF), 0.02, 0.3125, ((0, 4), (2, 32)))
    tokens = scatter_about(splits[2], (TOKENS, D), 1.0, 6.0, ((0, 128),))
    routes_keys = jax.random.split(jax.random.fold_in(splits[3], 1), TOKENS // TOK_DEV)
    routes_turns = jax.random.permutation(jax.random.fold_in(splits[3], 3), TOKENS // TOK_DEV)
    routes = jax.vmap(lambda own, number: routed_block(jax.random.fold_in(splits[3], 2), own, number, TOK_DEV, EXPERTS, TOP, CAP, 1))(routes_keys, routes_turns).reshape((TOKENS, TOP))
    router = scatter_about(splits[4], (D, EXPERTS), D ** -0.5, 0.09375)
    return {"attention_weights": attention_weights, "ffn_weights": ffn_weights, "tokens": tokens, "routes": routes, "router": router}


def slot_table(route_rows, experts_count, capacity):
    chosen = (route_rows[:, :, None] == jnp.arange(experts_count, dtype=jnp.int32)).astype(jnp.int32)
    flat_picks = chosen.reshape(-1, experts_count)
    before = jnp.cumsum(flat_picks, axis=0) - flat_picks
    position = jnp.sum(before * flat_picks, axis=1)
    slot_id = route_rows.reshape(-1) * capacity + position
    one_hot = (slot_id[:, None] == jnp.arange(experts_count * capacity, dtype=jnp.int32)).astype(jnp.float32)
    return jnp.sum(one_hot.reshape(route_rows.shape[0], route_rows.shape[1], -1), axis=1)


def expert_output(slot_rows, weights):
    gate_proj = jnp.dot(slot_rows, weights[0], preferred_element_type=jnp.float32)
    up_proj = jnp.dot(slot_rows, weights[1], preferred_element_type=jnp.float32)
    hidden = (jax.nn.silu(gate_proj) * up_proj).astype(jnp.bfloat16)
    part_width = FF // N_SHARD

    def add_part(summed, column):
        offset = column * part_width
        hidden_part = lax.dynamic_slice_in_dim(hidden, offset, part_width, 1)
        down_part = lax.dynamic_slice_in_dim(weights[2], offset, part_width, 1)
        partial_value = lax.dot_general(hidden_part, down_part, (((1,), (1,)), ((), ())), preferred_element_type=jnp.float32)
        rounded = lax.optimization_barrier(partial_value.astype(jnp.bfloat16))
        return summed + rounded.astype(jnp.float32), None

    initial = jnp.zeros((slot_rows.shape[0], weights.shape[1]), jnp.float32)
    summed, unused = lax.scan(add_part, initial, jnp.arange(N_SHARD, dtype=jnp.int32))
    return summed.astype(jnp.bfloat16)


def reference(attention_weights, ffn_weights, tokens, routes, router):
    attention_sum = jnp.sum(attention_weights.astype(jnp.float32), axis=0)
    merged_attention = (attention_sum * (1.0 / N_BRANCH)).astype(jnp.bfloat16)
    device_tokens = tokens.reshape(DEVICES, TOK_DEV, D)
    device_routes = routes.reshape(DEVICES, TOK_DEV, TOP)
    tables = jax.vmap(lambda route_rows: slot_table(route_rows, EXPERTS, CAP))(device_routes)
    buffers = jnp.einsum("dts,dtf->dsf", tables, device_tokens.astype(jnp.float32)).astype(jnp.bfloat16)
    per_expert = buffers.reshape(DEVICES, EXPERTS, CAP, D).transpose(1, 0, 2, 3).reshape(EXPERTS, DEVICES * CAP, D)
    results = lax.map(lambda expert_pair: expert_output(expert_pair[0], expert_pair[1]), (per_expert, ffn_weights))
    returned = results.reshape(EXPERTS, DEVICES, CAP, D).transpose(1, 0, 2, 3).reshape(DEVICES, EXPERTS * CAP, D)
    gates_all = jax.nn.sigmoid(jnp.dot(tokens, router, preferred_element_type=jnp.float32)).reshape(DEVICES, TOK_DEV, EXPERTS)
    weighting = tables * jnp.repeat(gates_all, CAP, axis=2)
    mixed_output = jnp.einsum("dts,dsf->dtf", weighting, returned.astype(jnp.float32), precision=lax.Precision.HIGHEST)
    mixed_output = mixed_output.astype(jnp.bfloat16).reshape(TOKENS, D)
    return merged_attention, ffn_weights, mixed_output
```

```python
import jax
import jax.numpy as jnp
from jax import lax
from jax.experimental import pallas as pl
from jax.experimental.pallas import tpu as pltpu
from jax.sharding import Mesh
from jax.sharding import PartitionSpec as P

MESH = pl.DeviceIdType.MESH
BF16 = jnp.bfloat16
F32 = jnp.float32

ROUNDS = []
for _a in (0, 1):
    ROUNDS += [
        [(1, 1, _a), (3, 3, 1 - _a)],
        [(1, 3, _a), (3, 1, 1 - _a)],
        [(1, 2, _a), (3, 0, 1 - _a)],
        [(3, 2, _a), (1, 0, 1 - _a)],
        [(2, 1, _a), (0, 3, 1 - _a)],
        [(2, 3, _a), (0, 1, 1 - _a)],
    ]
ROUNDS += [[(2, 2, 1)], [(2, 2, 0), (0, 0, 1)], [(2, 0, 1), (0, 2, 0)], [(2, 0, 0), (0, 2, 1)]]
ORDERS = (("x", "y", "z"), ("y", "z", "x"), ("z", "x", "y"))
WINDOW = 2


class Place:
    def __init__(self):
        self.y, self.x = lax.axis_index("y"), lax.axis_index("x")
        self.zh, self.zl = lax.axis_index("zh"), lax.axis_index("zl")
        self.core = lax.axis_index("core")
        self.z = self.zh * 2 + self.zl
        self.at = {"x": self.x, "y": self.y, "z": self.z}

    def shift(self, axis, k):
        return lax.rem(self.at[axis] + k, 4)

    def along(self, axis, k):
        v = self.shift(axis, k)
        if axis == "z":
            return {"zh": v // 2, "zl": lax.rem(v, 2)}
        return {axis: v}

    def shard(self, o):
        return lax.rem(self.y + o[0], 4), lax.rem(self.x + o[1], 4), lax.rem(self.zh + o[2], 2)


def block_index(place, order, phase, coords=None):
    done = order[:phase]
    out = []
    for axis in ("z", "y", "x"):
        if axis in done:
            out.append(slice(None))
        else:
            out.append(place.at[axis] if coords is None or axis not in coords else coords[axis])
    return tuple(out)


def gather_kernel(wt, tok, att, ew, tall, arecv, wbuf, tbuf, abuf, ws, wr, gs, gr, cs, cr, as_, ar, ls):
    p = Place()
    me = (p.y * 4 + p.x) * 2 + p.zh
    branch = p.zl * 2 + p.core
    units, width = ew.shape[1], wt.shape[2]
    rows = att.shape[1] // 4
    third = tok.shape[1] // 3

    bar = pltpu.get_barrier_semaphore()
    peers = []
    for r in ROUNDS:
        for o in r:
            a, b, c = p.shard(o)
            peers.append({"y": a, "x": b, "zh": c})
    peers += [p.along("z", 1), p.along("z", 3)]
    peers += [{"core": 1 - p.core}, {"zl": 1 - p.zl, "core": 1 - p.core}]
    for q in peers:
        pl.semaphore_signal(bar, inc=1, device_id=q, device_id_type=MESH)
    pl.semaphore_wait(bar, len(peers))

    def lanes(c):
        return pl.ds(c * third, third)

    def gather_copies(phase):
        out = []
        for c, order in enumerate(ORDERS):
            src_at = block_index(p, order, phase) + (p.core, slice(None), lanes(c))
            dst = tall.at[src_at]
            src = tok.at[:, lanes(c)] if phase == 0 else dst
            for k in (1, 3, 2):
                i = (phase * 3 + c) * 3 + k - 1
                out.append(
                    pltpu.make_async_remote_copy(
                        src, dst, gs.at[i], gr.at[i],
                        device_id=p.along(order[phase], k), device_id_type=MESH,
                    )
                )
        return out

    def weight_copies(number, r):
        out = []
        for j, o in enumerate(r):
            a, b, c = p.shard(o)
            d = (a * 4 + b) * 2 + c
            i = number * 2 + j
            out.append(
                pltpu.make_async_remote_copy(
                    wt.at[:, pl.ds(pl.multiple_of(d * units, 8), units), :],
                    ew.at[:, :, pl.ds(pl.multiple_of(me * width, 128), width)],
                    ws.at[i], wr.at[i],
                    device_id={"y": a, "x": b, "zh": c}, device_id_type=MESH,
                )
            )
        return out

    def att_copies():
        out = []
        for j, (dz, dc) in enumerate(((1, 0), (1, 1), (0, 1))):
            z2 = lax.rem(p.zl + dz, 2)
            c2 = lax.rem(p.core + dc, 2)
            b2 = z2 * 2 + c2
            out.append(
                pltpu.make_async_remote_copy(
                    att.at[:, pl.ds(pl.multiple_of(b2 * rows, 8), rows), :],
                    arecv.at[j], as_.at[j], ar.at[j],
                    device_id={"zl": z2, "core": c2}, device_id_type=MESH,
                )
            )
        return out

    def start(copies):
        for cp in copies:
            cp.start()

    phases = [gather_copies(ph) for ph in range(3)]
    rounds = [weight_copies(n, r) for n, r in enumerate(ROUNDS)]
    start(phases[0])
    start(rounds[0])
    start(rounds[1])

    own = [
        (wt.at[:, pl.ds(pl.multiple_of(me * units, 8), units), :], wbuf,
         ew.at[:, :, pl.ds(pl.multiple_of(me * width, 128), width)]),
        (tok, tbuf, tall.at[p.z, p.y, p.x, p.core]),
        (att.at[:, pl.ds(pl.multiple_of(branch * rows, 8), rows), :], abuf, arecv.at[3]),
    ]
    ins = [pltpu.make_async_copy(s, v, ls.at[i]) for i, (s, v, _) in enumerate(own)]
    outs = [pltpu.make_async_copy(v, d, ls.at[3 + i]) for i, (_, v, d) in enumerate(own)]
    start(ins)
    for i in range(3):
        ins[i].wait()
        outs[i].start()
    for cp in outs:
        cp.wait()

    swap = [
        pltpu.make_async_remote_copy(
            tall.at[:, :, :, p.core, :, lanes(c)], tall.at[:, :, :, p.core, :, lanes(c)],
            cs.at[c], cr.at[c], device_id={"core": 1 - p.core}, device_id_type=MESH,
        )
        for c in range(3)
    ]
    acopies = att_copies()

    for cp in phases[0]:
        cp.wait()
    start(phases[1])
    for n in range(2, len(rounds)):
        for cp in rounds[n - WINDOW]:
            cp.wait_send()
        start(rounds[n])
        if n == 4:
            for cp in phases[1]:
                cp.wait()
            start(phases[2])
        if n == 12:
            for cp in phases[2]:
                cp.wait()
            start(swap)
            start(acopies)
    for n in range(len(rounds) - WINDOW, len(rounds)):
        for cp in rounds[n]:
            cp.wait_send()
    for r in rounds:
        for cp in r:
            cp.wait_recv()
    for cp in swap + acopies:
        cp.wait()


def gather(wt, tok, att):
    units = wt.shape[1] // 32
    rows = att.shape[1] // 4
    dma = pltpu.SemaphoreType.DMA
    return pl.pallas_call(
        gather_kernel,
        out_shape=(
            jax.ShapeDtypeStruct((3, units, wt.shape[2] * 32), BF16),
            jax.ShapeDtypeStruct((4, 4, 4, 2) + tok.shape, BF16),
            jax.ShapeDtypeStruct((4, 2, rows, att.shape[2]), BF16),
        ),
        in_specs=[pl.BlockSpec(memory_space=pl.ANY)] * 3,
        out_specs=[pl.BlockSpec(memory_space=pl.ANY)] * 3,
        scratch_shapes=[
            pltpu.VMEM((3, units, wt.shape[2]), BF16),
            pltpu.VMEM(tok.shape, BF16),
            pltpu.VMEM((2, rows, att.shape[2]), BF16),
            dma((32,)), dma((32,)), dma((27,)), dma((27,)), dma((3,)), dma((3,)), dma((3,)), dma((3,)),
            dma((6,)),
        ],
        compiler_params=pltpu.CompilerParams(collective_id=0, has_side_effects=True),
    )(wt, tok, att)


def colour_lanes(width):
    tiles = width // 128
    cut = [0, -(-tiles // 3), -(-tiles // 3) + (tiles - tiles // 3) // 2, tiles]
    return [(cut[i] * 128, (cut[i + 1] - cut[i]) * 128) for i in range(3)]


def scatter_kernel(part, out, own, r0, s0, r1, s1, r2, s2, r3, ss, rs, ls):
    p = Place()
    bar = pltpu.get_barrier_semaphore()
    peers = [{"core": 1 - p.core}] + [p.along(a, k) for a in ("x", "y", "z") for k in (1, 2, 3)]
    for q in peers:
        pl.semaphore_signal(bar, inc=1, device_id=q, device_id_type=MESH)
    pl.semaphore_wait(bar, len(peers))
    cuts = colour_lanes(part.shape[5])

    swaps, loads = [], []
    for c, (lo, n) in enumerate(cuts):
        swaps.append(
            pltpu.make_async_remote_copy(
                part.at[:, :, :, 1 - p.core, :, pl.ds(lo, n)], r0[c],
                ss.at[c], rs.at[c], device_id={"core": 1 - p.core}, device_id_type=MESH,
            )
        )
        loads.append(
            pltpu.make_async_copy(part.at[:, :, :, p.core, :, pl.ds(lo, n)], own[c], ls.at[c])
        )
    for a, b in zip(swaps, loads):
        a.start()
        b.start()

    stage1, stage2, stage3 = [], [], []

    def send(stage, c, axis, src_of, dst):
        copies = []
        for k in (1, 3, 2):
            i = 3 + (stage * 3 + c) * 3 + k - 1
            cp = pltpu.make_async_remote_copy(
                src_of(p.shift(axis, k)), dst.at[k - 1], ss.at[i], rs.at[i],
                device_id=p.along(axis, k), device_id_type=MESH,
            )
            cp.start()
            copies.append(cp)
        return copies

    def pick(ref, left, axis, v):
        return ref.at[tuple(v if a == axis else slice(None) for a in left)]

    def left_after(order, phase):
        return [a for a in ("z", "y", "x") if a not in order[:phase]]

    for c, order in enumerate(ORDERS):
        swaps[c].wait()
        loads[c].wait()

        def add(i, carry, c=c):
            at = (i // 16, lax.rem(i // 4, 4), lax.rem(i, 4))
            s0[c][at] = (own[c][at].astype(F32) + r0[c][at].astype(F32)).astype(BF16)
            return carry

        lax.fori_loop(0, 64, add, 0)
        left = left_after(order, 0)
        stage1.append(send(0, c, order[0], lambda v, c=c, left=left, a=order[0]: pick(s0[c], left, a, v), r1[c]))

    for c, order in enumerate(ORDERS):
        for cp in stage1[c]:
            cp.wait()
        mine = pick(s0[c], left_after(order, 0), order[0], p.at[order[0]])

        def add(i, carry, c=c, mine=mine):
            at = (i // 4, lax.rem(i, 4))
            total = mine[at].astype(F32)
            for k in range(3):
                total += r1[c][(k,) + at].astype(F32)
            s1[c][at] = total.astype(BF16)
            return carry

        lax.fori_loop(0, 16, add, 0)
        left = left_after(order, 1)
        stage2.append(send(1, c, order[1], lambda v, c=c, left=left, a=order[1]: pick(s1[c], left, a, v), r2[c]))

    for c, order in enumerate(ORDERS):
        for cp in stage2[c]:
            cp.wait()
        mine = pick(s1[c], left_after(order, 1), order[1], p.at[order[1]])

        def add(i, carry, c=c, mine=mine):
            total = mine[i].astype(F32)
            for k in range(3):
                total += r2[c][k, i].astype(F32)
            s2[c][i] = total.astype(BF16)
            return carry

        lax.fori_loop(0, 4, add, 0)
        left = left_after(order, 2)
        stage3.append(send(2, c, order[2], lambda v, c=c, left=left, a=order[2]: pick(s2[c], left, a, v), r3[c]))

    for c, order in enumerate(ORDERS):
        for cp in stage3[c]:
            cp.wait()
        total = s2[c][p.at[order[2]]].astype(F32)
        for k in range(3):
            total += r3[c][k].astype(F32)
        lo, n = cuts[c]
        out[:, lo:lo + n] = total.astype(BF16)


def scatter(part):
    rows, width = part.shape[4:]
    cuts = colour_lanes(width)
    dma = pltpu.SemaphoreType.DMA

    def bufs(*lead):
        return [pltpu.VMEM(lead + (rows, n), BF16) for _, n in cuts]

    return pl.pallas_call(
        scatter_kernel,
        out_shape=jax.ShapeDtypeStruct((rows, width), BF16),
        in_specs=[pl.BlockSpec(memory_space=pl.ANY)],
        out_specs=pl.BlockSpec(memory_space=pltpu.VMEM),
        scratch_shapes=[
            bufs(4, 4, 4), bufs(4, 4, 4), bufs(4, 4, 4),
            bufs(3, 4, 4), bufs(4, 4), bufs(3, 4), bufs(4), bufs(3),
            dma((30,)), dma((30,)), dma((3,)),
        ],
        compiler_params=pltpu.CompilerParams(
            collective_id=1, has_side_effects=True, vmem_limit_bytes=56 * 1024 * 1024
        ),
    )(part)


def local(attention_weights, ffn_weights, tokens, routes, router):
    experts = router.shape[1]
    width = tokens.shape[1]
    wt = jnp.swapaxes(ffn_weights[0], 1, 2)
    gates = jax.nn.sigmoid(jnp.dot(tokens, router, preferred_element_type=F32))
    named = jnp.sum((routes[:, :, None] == jnp.arange(experts, dtype=jnp.int32)).astype(F32), axis=1)
    weighting = named * gates
    high = lax.reduce_precision(weighting, 8, 7)
    low = (weighting - high).astype(BF16)
    high = high.astype(BF16)
    tok = jnp.concatenate(
        [tokens, high, low, jnp.zeros((tokens.shape[0], 128 - 2 * experts), BF16)], axis=1
    )
    ew, tall, arecv = gather(wt, tok, attention_weights[0])
    flat = tall.reshape(-1, tok.shape[1])
    rows = flat[:, :width]
    expert = lax.axis_index("zl") * 2 + lax.axis_index("core")
    pair = lax.dynamic_slice_in_dim(flat[:, width:width + experts], expert, 1, 1).astype(F32)
    pair += lax.dynamic_slice_in_dim(flat[:, width + experts:width + 2 * experts], expert, 1, 1).astype(F32)
    nt = (((1,), (1,)), ((), ()))
    gate_proj = lax.dot_general(rows, ew[0], nt, preferred_element_type=F32)
    up_proj = lax.dot_general(rows, ew[1], nt, preferred_element_type=F32)
    hidden = (jax.nn.silu(gate_proj) * up_proj * pair).astype(BF16)
    part = jnp.dot(hidden, ew[2], preferred_element_type=F32).astype(BF16)
    mixed_output = scatter(part.reshape(tall.shape[:5] + (width,)))
    merged = (jnp.sum(arecv.astype(F32), axis=0) * 0.25).astype(BF16)
    return merged, jnp.swapaxes(ew, 1, 2)[None], mixed_output


def solution(mesh):
    torus = Mesh(mesh.devices.reshape(2, 2, 4, 4, 2), ("zl", "core", "y", "x", "zh"))
    shard = ("y", "x", "zh")
    branch = ("zl", "core")
    in_specs = (
        P(branch, None, None, shard),
        P(branch, None, shard, None),
        P(branch + shard, None),
        P(branch + shard, None),
        P(),
    )
    out_specs = (P(None, branch, shard), P(branch, None, None, shard), P(branch + shard, None))
    return jax.shard_map(local, mesh=torus, in_specs=in_specs, out_specs=out_specs, check_vma=False)
```

```python
import jax
import jax.numpy as jnp
from jax import lax
from jax.experimental import pallas as pl
from jax.experimental.pallas import tpu as pltpu
from jax.sharding import Mesh
from jax.sharding import PartitionSpec as P

MESH = pl.DeviceIdType.MESH
BF16 = jnp.bfloat16
F32 = jnp.float32

PATHS = (("zh", "x", "y"), ("y", "zh", "x"), ("x", "y", "zh"))
SIZE = {"y": 4, "x": 4, "zh": 2}
GRID = ("y", "x", "zh")
ORDERS = (("x", "y", "z"), ("y", "z", "x"), ("z", "x", "y"))


class Place:
    def __init__(self):
        self.y, self.x = lax.axis_index("y"), lax.axis_index("x")
        self.zh, self.zl = lax.axis_index("zh"), lax.axis_index("zl")
        self.core = lax.axis_index("core")
        self.z = self.zh * 2 + self.zl
        self.at = {"x": self.x, "y": self.y, "z": self.z}

    def shift(self, axis, k):
        return lax.rem(self.at[axis] + k, 4)

    def along(self, axis, k):
        v = self.shift(axis, k)
        if axis == "z":
            return {"zh": v // 2, "zl": lax.rem(v, 2)}
        return {axis: v}

    def shard(self, o):
        return lax.rem(self.y + o[0], 4), lax.rem(self.x + o[1], 4), lax.rem(self.zh + o[2], 2)


def block_index(place, order, phase, coords=None):
    done = order[:phase]
    out = []
    for axis in ("z", "y", "x"):
        if axis in done:
            out.append(slice(None))
        else:
            out.append(place.at[axis] if coords is None or axis not in coords else coords[axis])
    return tuple(out)


def gather_kernel(wt, tok, att, ew, tall, arecv, b1, b2, tbuf, abuf,
                  s1, r1, s2, r2, s3, r3, gs, gr, cs, cr, as_, ar, ls):
    p = Place()
    branch = p.zl * 2 + p.core
    rows = att.shape[1] // 4
    third = tok.shape[1] // 3
    pos = {"y": p.y, "x": p.x, "zh": p.zh}

    def near(axis, k):
        return lax.rem(pos[axis] + k, SIZE[axis])

    bar = pltpu.get_barrier_semaphore()
    peers = [p.along(a, k) for a in ("x", "y", "z") for k in (1, 2, 3)]
    peers += [{"core": 1 - p.core}, {"zl": 1 - p.zl, "core": 1 - p.core}]
    for q in peers:
        pl.semaphore_signal(bar, inc=1, device_id=q, device_id_type=MESH)
    pl.semaphore_wait(bar, len(peers))

    def start(copies):
        for cp in copies:
            cp.start()

    def lanes(c):
        return pl.ds(c * third, third)

    def gather_copies(phase):
        out = []
        for c, order in enumerate(ORDERS):
            dst = tall.at[(p.core,) + block_index(p, order, phase) + (slice(None), lanes(c))]
            src = tok.at[:, lanes(c)] if phase == 0 else dst
            for k in (1, 3, 2):
                i = (phase * 3 + c) * 3 + k - 1
                out.append(
                    pltpu.make_async_remote_copy(
                        src, dst, gs.at[i], gr.at[i],
                        device_id=p.along(order[phase], k), device_id_type=MESH,
                    )
                )
        return out

    def att_copies():
        out = []
        for j, (dz, dc) in enumerate(((1, 0), (1, 1), (0, 1))):
            z2 = lax.rem(p.zl + dz, 2)
            c2 = lax.rem(p.core + dc, 2)
            b2_ = z2 * 2 + c2
            out.append(
                pltpu.make_async_remote_copy(
                    att.at[:, pl.ds(pl.multiple_of(b2_ * rows, 8), rows), :],
                    arecv.at[j], as_.at[j], ar.at[j],
                    device_id={"zl": z2, "core": c2}, device_id_type=MESH,
                )
            )
        return out

    def blocks(ref, **fixed):
        return ref.at[tuple(fixed.get(a, slice(None)) for a in GRID)]

    def remote(src, dst, send, recv, axis, k):
        return pltpu.make_async_remote_copy(
            src, dst, send, recv, device_id={axis: near(axis, k)}, device_id_type=MESH
        )

    def hops(axis):
        return (1, 3, 2) if SIZE[axis] == 4 else (1,)

    def column(ref, m, y, x, zh):
        lane = ((y * 4 + x) * 2 + zh) * 128
        return ref.at[m, :, pl.ds(pl.multiple_of(lane, 128), 128)]

    step1, step2, step3, keep = {}, {}, {}, []
    number2 = number3 = 0
    for m, (a, b, c) in enumerate(PATHS):
        for k in hops(a):
            step1[m, k] = remote(
                blocks(wt.at[m], **{a: near(a, k)}), blocks(b1.at[m], **{a: pos[a]}),
                s1.at[m * 3 + k - 1], r1.at[m * 3 + k - 1], a, k,
            )
        for i in range(SIZE[a]):
            src_a = near(a, SIZE[a] - i)
            for k in hops(b):
                step2[m, i, k] = remote(
                    blocks(b1.at[m], **{a: src_a, b: near(b, k)}),
                    blocks(b2.at[m], **{a: src_a, b: pos[b]}),
                    s2.at[number2], r2.at[number2], b, k,
                )
                number2 += 1
            for j in range(SIZE[b]):
                src_b = near(b, SIZE[b] - j)
                held = b1 if j == 0 else b2
                for k in hops(c):
                    step3[m, i, j, k] = remote(
                        blocks(held.at[m], **{a: src_a, b: src_b, c: near(c, k)}),
                        column(ew, m, **{a: src_a, b: src_b, c: pos[c]}),
                        s3.at[number3], r3.at[number3], c, k,
                    )
                    number3 += 1
                keep.append(
                    (m, i, j, pltpu.make_async_copy(
                        blocks(held.at[m], **{a: src_a, b: src_b, c: pos[c]}),
                        column(ew, m, **{a: src_a, b: src_b, c: pos[c]}),
                        ls.at[10 + len(keep)],
                    ))
                )
    keep = {(m, i, j): cp for m, i, j, cp in keep}

    phases = [gather_copies(ph) for ph in range(3)]
    swap = [
        pltpu.make_async_remote_copy(
            tall.at[p.core, :, :, :, :, lanes(c)], tall.at[p.core, :, :, :, :, lanes(c)],
            cs.at[c], cr.at[c], device_id={"core": 1 - p.core}, device_id_type=MESH,
        )
        for c in range(3)
    ]
    acopies = att_copies()

    start(phases[0])
    start(step1.values())
    start(acopies)

    local_in = [
        pltpu.make_async_copy(blocks(wt.at[m], **{a: pos[a]}), blocks(b1.at[m], **{a: pos[a]}), ls.at[m])
        for m, (a, _, _) in enumerate(PATHS)
    ]
    own = [
        (tok, tbuf, tall.at[p.core, p.z, p.y, p.x]),
        (att.at[:, pl.ds(pl.multiple_of(branch * rows, 8), rows), :], abuf, arecv.at[3]),
    ]
    ins = [pltpu.make_async_copy(s, v, ls.at[3 + i]) for i, (s, v, _) in enumerate(own)]
    outs = [pltpu.make_async_copy(v, d, ls.at[5 + i]) for i, (_, v, d) in enumerate(own)]
    start(local_in)
    start(ins)
    for i in range(2):
        ins[i].wait()
        outs[i].start()
    for cp in local_in + outs:
        cp.wait()

    for cp in phases[0]:
        cp.wait()
    start(phases[1])
    for m in range(3):
        start(step2[m, 0, k] for k in hops(PATHS[m][1]))
    for i in (1, 3, 2):
        for m in range(3):
            if i in hops(PATHS[m][0]):
                step1[m, i].wait()
                start(step2[m, i, k] for k in hops(PATHS[m][1]))
        if i == 1:
            for cp in phases[1]:
                cp.wait()
            start(phases[2])
    for i in (0, 1, 3, 2):
        for m in range(3):
            if i < SIZE[PATHS[m][0]]:
                start(step3[m, i, 0, k] for k in hops(PATHS[m][2]))
                keep[m, i, 0].start()
    for i in (0, 1, 3, 2):
        for j in (1, 3, 2):
            for m in range(3):
                if i < SIZE[PATHS[m][0]] and j in hops(PATHS[m][1]):
                    step2[m, i, j].wait()
                    start(step3[m, i, j, k] for k in hops(PATHS[m][2]))
                    keep[m, i, j].start()
        if i == 1:
            for cp in phases[2]:
                cp.wait()
            start(swap)
    for cp in acopies + swap + list(keep.values()) + list(step3.values()):
        cp.wait()


def gather(wt, tok, att):
    units, depth = wt.shape[4:]
    rows = att.shape[1] // 4
    dma = pltpu.SemaphoreType.DMA
    return pl.pallas_call(
        gather_kernel,
        out_shape=(
            jax.ShapeDtypeStruct((3, units, depth * 32), BF16),
            jax.ShapeDtypeStruct((2, 4, 4, 4) + tok.shape, BF16),
            jax.ShapeDtypeStruct((4, 2, rows, att.shape[2]), BF16),
        ),
        in_specs=[pl.BlockSpec(memory_space=pl.ANY)] * 3,
        out_specs=[pl.BlockSpec(memory_space=pl.ANY)] * 3,
        scratch_shapes=[
            pltpu.VMEM(wt.shape, BF16),
            pltpu.VMEM(wt.shape, BF16),
            pltpu.VMEM(tok.shape, BF16),
            pltpu.VMEM((2, rows, att.shape[2]), BF16),
            dma((9,)), dma((9,)), dma((24,)), dma((24,)), dma((64,)), dma((64,)),
            dma((27,)), dma((27,)), dma((3,)), dma((3,)), dma((3,)), dma((3,)), dma((48,)),
        ],
        compiler_params=pltpu.CompilerParams(
            collective_id=0, has_side_effects=True, vmem_limit_bytes=40 * 1024 * 1024
        ),
    )(wt, tok, att)


def colour_lanes(width):
    tiles = width // 128
    cut = [0, -(-tiles // 3), -(-tiles // 3) + (tiles - tiles // 3) // 2, tiles]
    return [(cut[i] * 128, (cut[i + 1] - cut[i]) * 128) for i in range(3)]


def hidden_kernel(rows, ew, hid, copy, wv, sems):
    step = pl.program_id(0)
    units, width = ew.shape[1:]
    loads = [pltpu.make_async_copy(ew.at[m], wv.at[m, pl.ds(0, units)], sems.at[m]) for m in range(3)]
    stores = [pltpu.make_async_copy(wv.at[m, pl.ds(0, units)], copy.at[m], sems.at[3 + m]) for m in range(3)]

    @pl.when(step == 0)
    def _():
        for cp in loads:
            cp.start()
        for m in range(3):
            loads[m].wait()
            stores[m].start()

    both = wv[0:2].reshape(2 * wv.shape[1], width)
    proj = lax.dot_general(
        rows[:, :width], both, (((1,), (1,)), ((), ())), preferred_element_type=F32
    )
    gate, up = proj[:, :wv.shape[1]], proj[:, wv.shape[1]:]
    extra = rows[:, width:].astype(F32)
    lane = lax.broadcasted_iota(jnp.int32, extra.shape, 1)
    expert = lax.axis_index("zl") * 2 + lax.axis_index("core")
    mine = (lane == expert) | (lane == expert + 4)
    weight = jnp.sum(jnp.where(mine, extra, 0.0), axis=1, keepdims=True)
    value = gate / (1.0 + jnp.exp(-gate)) * up * weight
    hid[...] = value[:, :units].astype(BF16)

    @pl.when(step == pl.num_programs(0) - 1)
    def _():
        for cp in stores:
            cp.wait()


def hidden_of(rows, ew):
    count, units = 256, ew.shape[1]
    return pl.pallas_call(
        hidden_kernel,
        grid=(rows.shape[0] // count,),
        out_shape=(
            jax.ShapeDtypeStruct((rows.shape[0], units), BF16),
            jax.ShapeDtypeStruct(ew.shape, BF16),
        ),
        in_specs=[
            pl.BlockSpec((count, rows.shape[1]), lambda i: (i, 0)),
            pl.BlockSpec(memory_space=pl.ANY),
        ],
        out_specs=[
            pl.BlockSpec((count, units), lambda i: (i, 0)),
            pl.BlockSpec(memory_space=pl.ANY),
        ],
        scratch_shapes=[
            pltpu.VMEM((3, -(-units // 128) * 128, ew.shape[2]), BF16),
            pltpu.SemaphoreType.DMA((6,)),
        ],
        compiler_params=pltpu.CompilerParams(vmem_limit_bytes=40 * 1024 * 1024),
    )(rows, ew)


CHUNKS = (1, 3, 2, 0)


def scatter_kernel(hid, ew, out, down, snd, r0, s0, r1, s1, r2, s2, r3, xs, xr, ss, rs, ls):
    p = Place()
    load = pltpu.make_async_copy(ew.at[2], down, ls)
    load.start()
    bar = pltpu.get_barrier_semaphore()
    peers = [{"core": 1 - p.core}] + [p.along(a, k) for a in ("x", "y", "z") for k in (1, 2, 3)]
    for q in peers:
        pl.semaphore_signal(bar, inc=1, device_id=q, device_id_type=MESH)
    pl.semaphore_wait(bar, len(peers))
    load.wait()
    cuts = colour_lanes(down.shape[1])

    def product(core, z, c):
        lo, n = cuts[c]
        rows = hid[core, z].reshape(-1, hid.shape[-1])
        value = jnp.dot(rows, down[:, lo:lo + n], preferred_element_type=F32)
        return value.reshape(4, 4, -1, n)

    def swap(j, c):
        z = p.shift("z", j)
        return pltpu.make_async_remote_copy(
            snd[c].at[z], r0[c].at[z], xs.at[j * 3 + c], xr.at[j * 3 + c],
            device_id={"core": 1 - p.core}, device_id_type=MESH,
        )

    swaps = {(j, c): swap(j, c) for j in range(4) for c in range(3)}
    number = iter(range(60))

    def remote(src, dst, axis, k):
        i = next(number)
        return pltpu.make_async_remote_copy(
            src, dst, ss.at[i], rs.at[i], device_id=p.along(axis, k), device_id_type=MESH
        )

    def give(j):
        z = p.shift("z", j)
        for c in range(3):
            snd[c][z] = product(1 - p.core, z, c).astype(BF16)
            swaps[j, c].start()

    stage1 = [[], [], []]

    def take(j):
        z = p.shift("z", j)
        for c, order in enumerate(ORDERS):
            value = product(p.core, z, c)
            swaps[j, c].wait()
            s0[c][z] = (value + r0[c][z].astype(F32)).astype(BF16)
            axis = order[0]
            if axis == "z":
                copies = [remote(s0[c].at[z], r1[c].at[j - 1], "z", j)] if j else []
            elif axis == "y":
                copies = [
                    remote(s0[c].at[z, p.shift("y", k)], r1[c].at[k - 1, z], "y", k) for k in (1, 3, 2)
                ]
            else:
                copies = [
                    remote(s0[c].at[z, :, p.shift("x", k)], r1[c].at[k - 1, z], "x", k) for k in (1, 3, 2)
                ]
            for cp in copies:
                cp.start()
            stage1[c] += copies

    give(CHUNKS[0])
    for n in range(4):
        if n < 3:
            give(CHUNKS[n + 1])
        take(CHUNKS[n])

    def pick(ref, left, axis, v):
        return ref.at[tuple(v if a == axis else slice(None) for a in left)]

    def left_after(order, phase):
        return [a for a in ("z", "y", "x") if a not in order[:phase]]

    def send(c, axis, src_of, dst):
        copies = [remote(src_of(p.shift(axis, k)), dst.at[k - 1], axis, k) for k in (1, 3, 2)]
        for cp in copies:
            cp.start()
        return copies

    stage2, stage3 = [], []
    for c, order in enumerate(ORDERS):
        for cp in stage1[c]:
            cp.wait()
        mine = pick(s0[c], left_after(order, 0), order[0], p.at[order[0]])

        def add(i, carry, c=c, mine=mine):
            at = (i // 4, lax.rem(i, 4))
            total = mine[at].astype(F32)
            for k in range(3):
                total += r1[c][(k,) + at].astype(F32)
            s1[c][at] = total.astype(BF16)
            return carry

        lax.fori_loop(0, 16, add, 0)
        left = left_after(order, 1)
        stage2.append(send(c, order[1], lambda v, c=c, left=left, a=order[1]: pick(s1[c], left, a, v), r2[c]))

    for c, order in enumerate(ORDERS):
        for cp in stage2[c]:
            cp.wait()
        mine = pick(s1[c], left_after(order, 1), order[1], p.at[order[1]])

        def add(i, carry, c=c, mine=mine):
            total = mine[i].astype(F32)
            for k in range(3):
                total += r2[c][k, i].astype(F32)
            s2[c][i] = total.astype(BF16)
            return carry

        lax.fori_loop(0, 4, add, 0)
        left = left_after(order, 2)
        stage3.append(send(c, order[2], lambda v, c=c, left=left, a=order[2]: pick(s2[c], left, a, v), r3[c]))

    for c, order in enumerate(ORDERS):
        for cp in stage3[c]:
            cp.wait()
        total = s2[c][p.at[order[2]]].astype(F32)
        for k in range(3):
            total += r3[c][k].astype(F32)
        lo, n = cuts[c]
        out[:, lo:lo + n] = total.astype(BF16)


def scatter(hid, ew):
    rows, units = hid.shape[-2:]
    width = ew.shape[2]
    cuts = colour_lanes(width)
    dma = pltpu.SemaphoreType.DMA

    def bufs(*lead):
        return [pltpu.VMEM(lead + (rows, n), BF16) for _, n in cuts]

    return pl.pallas_call(
        scatter_kernel,
        out_shape=jax.ShapeDtypeStruct((rows, width), BF16),
        in_specs=[pl.BlockSpec(memory_space=pltpu.VMEM), pl.BlockSpec(memory_space=pl.ANY)],
        out_specs=pl.BlockSpec(memory_space=pltpu.VMEM),
        scratch_shapes=[
            pltpu.VMEM((units, width), BF16),
            bufs(4, 4, 4), bufs(4, 4, 4), bufs(4, 4, 4),
            bufs(3, 4, 4), bufs(4, 4), bufs(3, 4), bufs(4), bufs(3),
            dma((12,)), dma((12,)), dma((60,)), dma((60,)), dma,
        ],
        compiler_params=pltpu.CompilerParams(
            collective_id=1, has_side_effects=True, vmem_limit_bytes=56 * 1024 * 1024
        ),
    )(hid, ew)


def local(attention_weights, ffn_weights, tokens, routes, router):
    experts = router.shape[1]
    width = tokens.shape[1]
    wt = jnp.swapaxes(ffn_weights[0], 1, 2)
    wt = wt.reshape(3, 4, 4, 2, wt.shape[1] // 32, wt.shape[2])
    gates = jax.nn.sigmoid(jnp.dot(tokens, router, preferred_element_type=F32))
    named = jnp.sum((routes[:, :, None] == jnp.arange(experts, dtype=jnp.int32)).astype(F32), axis=1)
    weighting = named * gates
    high = lax.reduce_precision(weighting, 8, 7)
    low = (weighting - high).astype(BF16)
    high = high.astype(BF16)
    tok = jnp.concatenate(
        [tokens, high, low, jnp.zeros((tokens.shape[0], 128 - 2 * experts), BF16)], axis=1
    )
    ew, tall, arecv = gather(wt, tok, attention_weights[0])
    flat = tall.reshape(-1, tok.shape[1])
    hid, kept = hidden_of(flat, ew)
    mixed_output = scatter(hid.reshape(2, 4, 4, 4, tokens.shape[0], -1), kept)
    merged = (jnp.sum(arecv.astype(F32), axis=0) * 0.25).astype(BF16)
    return merged, jnp.swapaxes(kept, 1, 2)[None], mixed_output


def solution(mesh):
    torus = Mesh(mesh.devices.reshape(2, 2, 4, 4, 2), ("zl", "core", "y", "x", "zh"))
    shard = ("y", "x", "zh")
    branch = ("zl", "core")
    in_specs = (
        P(branch, None, None, shard),
        P(branch, None, shard, None),
        P(branch + shard, None),
        P(branch + shard, None),
        P(),
    )
    out_specs = (P(None, branch, shard), P(branch, None, None, shard), P(branch + shard, None))
    return jax.shard_map(local, mesh=torus, in_specs=in_specs, out_specs=out_specs, check_vma=False)
```

```python
import jax
import jax.numpy as jnp
from jax import lax
from jax.experimental import pallas as pl
from jax.experimental.pallas import tpu as pltpu
from jax.sharding import Mesh
from jax.sharding import PartitionSpec as P

MESH = pl.DeviceIdType.MESH
BF16 = jnp.bfloat16
F32 = jnp.float32

PATHS = (("zh", "x", "y"), ("y", "zh", "x"), ("x", "y", "zh"))
SIZE = {"y": 4, "x": 4, "zh": 2}
GRID = ("y", "x", "zh")
ORDERS = (("x", "y", "z"), ("y", "z", "x"), ("z", "x", "y"))


class Place:
    def __init__(self):
        self.y, self.x = lax.axis_index("y"), lax.axis_index("x")
        self.zh, self.zl = lax.axis_index("zh"), lax.axis_index("zl")
        self.core = lax.axis_index("core")
        self.z = self.zh * 2 + self.zl
        self.at = {"x": self.x, "y": self.y, "z": self.z}

    def shift(self, axis, k):
        return lax.rem(self.at[axis] + k, 4)

    def along(self, axis, k):
        v = self.shift(axis, k)
        if axis == "z":
            return {"zh": v // 2, "zl": lax.rem(v, 2)}
        return {axis: v}

    def shard(self, o):
        return lax.rem(self.y + o[0], 4), lax.rem(self.x + o[1], 4), lax.rem(self.zh + o[2], 2)


def block_index(place, order, phase, coords=None):
    done = order[:phase]
    out = []
    for axis in ("z", "y", "x"):
        if axis in done:
            out.append(slice(None))
        else:
            out.append(place.at[axis] if coords is None or axis not in coords else coords[axis])
    return tuple(out)


def gather_kernel(w, tok, att, ew, tall, near_sum, far_sum, raw, wt, b1, b2, turned, tbuf, aown, arecv,
                  s1, r1, s2, r2, s3, r3, gs, gr, cs, cr, as_, ar, ls):
    p = Place()
    rows = att.shape[1] // 4
    third = tok.shape[1] // 3
    units = ew.shape[1]
    pos = {"y": p.y, "x": p.x, "zh": p.zh}

    def near(axis, k):
        return lax.rem(pos[axis] + k, SIZE[axis])

    def start(copies):
        for cp in copies:
            cp.start()

    loads = [pltpu.make_async_copy(w.at[m], raw.at[m], ls.at[m]) for m in range(3)]
    tin = pltpu.make_async_copy(tok, tbuf, ls.at[3])
    tout = pltpu.make_async_copy(tbuf, tall.at[p.core, p.z, p.y, p.x], ls.at[4])
    tin.start()
    start(loads)
    ours = [
        pltpu.make_async_copy(
            att.at[:, pl.ds(pl.multiple_of((z * 2 + p.core) * rows, 8), rows), :], aown.at[z], ls.at[45 + z]
        )
        for z in range(2)
    ]
    start(ours)

    bar = pltpu.get_barrier_semaphore()
    peers = [p.along(a, k) for a in ("x", "y", "z") for k in (1, 2, 3)]
    peers += [{"core": 1 - p.core}]
    for q in peers:
        pl.semaphore_signal(bar, inc=1, device_id=q, device_id_type=MESH)
    pl.semaphore_wait(bar, len(peers))

    def lanes(c):
        return pl.ds(c * third, third)

    def gather_copies(phase, hops_):
        out = []
        for c, order in enumerate(ORDERS):
            dst = tall.at[(p.core,) + block_index(p, order, phase) + (slice(None), lanes(c))]
            src = tok.at[:, lanes(c)] if phase == 0 else dst
            for k in hops_:
                i = (phase * 3 + c) * 3 + k - 1
                out.append(
                    pltpu.make_async_remote_copy(
                        src, dst, gs.at[i], gr.at[i],
                        device_id=p.along(order[phase], k), device_id_type=MESH,
                    )
                )
        return out

    def relay_copies(back):
        out = []
        for c, order in enumerate(ORDERS):
            axis = order[2]
            at = list(block_index(p, order, 2, {axis: p.shift(axis, 4 - back)}))
            split = [n for n in range(3) if isinstance(at[n], slice)][0]
            at[split] = pl.ds(0 if back == 1 else 2, 2)
            ref = tall.at[(p.core,) + tuple(at) + (slice(None), lanes(c))]
            i = 27 + c * 2 + (0 if back == 1 else 1)
            out.append(
                pltpu.make_async_remote_copy(
                    ref, ref, gs.at[i], gr.at[i],
                    device_id=p.along(axis, back), device_id_type=MESH,
                )
            )
        return out

    def blocks(ref, **fixed):
        return ref.at[tuple(fixed.get(a, slice(None)) for a in GRID)]

    def remote(src, dst, send, recv, axis, k):
        return pltpu.make_async_remote_copy(
            src, dst, send, recv, device_id={axis: near(axis, k)}, device_id_type=MESH
        )

    def hops(axis):
        return (1, 3, 2) if SIZE[axis] == 4 else (1,)

    def column(ref, m, y, x, zh):
        lane = ((y * 4 + x) * 2 + zh) * 128
        return ref.at[m, :, pl.ds(pl.multiple_of(lane, 128), 128)]

    step1, step2, step3, keep = {}, {}, {}, {}
    number2 = number3 = 0
    for m, (a, b, c) in enumerate(PATHS):
        for k in hops(a):
            step1[m, k] = remote(
                blocks(wt.at[m], **{a: near(a, k)}), blocks(b1.at[m], **{a: pos[a]}),
                s1.at[m * 3 + k - 1], r1.at[m * 3 + k - 1], a, k,
            )
        for i in range(SIZE[a]):
            src_a = near(a, SIZE[a] - i)
            first = wt if i == 0 else b1
            for k in hops(b):
                step2[m, i, k] = remote(
                    blocks(first.at[m], **{a: src_a, b: near(b, k)}),
                    blocks(b2.at[m], **{a: src_a, b: pos[b]}),
                    s2.at[number2], r2.at[number2], b, k,
                )
                number2 += 1
            for j in range(SIZE[b]):
                src_b = near(b, SIZE[b] - j)
                held = first if j == 0 else b2
                for k in hops(c):
                    step3[m, i, j, k] = remote(
                        blocks(held.at[m], **{a: src_a, b: src_b, c: near(c, k)}),
                        column(ew, m, **{a: src_a, b: src_b, c: pos[c]}),
                        s3.at[number3], r3.at[number3], c, k,
                    )
                    number3 += 1
                keep[m, i, j] = pltpu.make_async_copy(
                    blocks(held.at[m], **{a: src_a, b: src_b, c: pos[c]}),
                    column(ew, m, **{a: src_a, b: src_b, c: pos[c]}),
                    ls.at[5 + len(keep)],
                )

    phase0, phase1 = gather_copies(0, (1, 3, 2)), gather_copies(1, (1, 3, 2))
    phase2a, phase2b = gather_copies(2, (1,)), gather_copies(2, (3,))
    relay_a, relay_b = relay_copies(1), relay_copies(3)
    def swap_copies(k):
        out = []
        for c, order in enumerate(ORDERS):
            at = block_index(p, order, 2, {order[2]: p.shift(order[2], 4 - k)})
            ref = tall.at[(p.core,) + at + (slice(None), lanes(c))]
            out.append(
                pltpu.make_async_remote_copy(
                    ref, ref, cs.at[c * 4 + k], cr.at[c * 4 + k],
                    device_id={"core": 1 - p.core}, device_id_type=MESH,
                )
            )
        return out

    swaps = [swap_copies(k) for k in range(4)]
    acopies = [
        pltpu.make_async_remote_copy(
            att.at[:, pl.ds(pl.multiple_of((z * 2 + 1 - p.core) * rows, 8), rows), :],
            arecv.at[z], as_.at[z], ar.at[z],
            device_id={"core": 1 - p.core}, device_id_type=MESH,
        )
        for z in range(2)
    ]

    start(phase0)
    start(acopies)
    tin.wait()
    tout.start()
    tout.wait()

    def turn(m):
        def body(i, carry):
            at = pl.ds(pl.multiple_of(i * 256, 256), 256)
            turned[at, :] = raw[m, :, at].T.astype(F32)
            return carry

        def place(d, carry):
            piece = turned[pl.ds(pl.multiple_of(d * units, 8), units), :]
            wt[m, d // 8, lax.rem(d // 2, 4), lax.rem(d, 2)] = piece.astype(BF16)
            return carry

        lax.fori_loop(0, raw.shape[2] // 256, body, 0, unroll=2)
        lax.fori_loop(0, 32, place, 0, unroll=4)

    for m in range(3):
        loads[m].wait()
        turn(m)
        start(step1[m, k] for k in hops(PATHS[m][0]))
        if m == 0:
            for cp in phase0:
                cp.wait()
            start(phase1)
        if m == 2:
            for cp in phase1:
                cp.wait()
            start(phase2a)
            start(phase2b)
            start(swaps[0])
    for m in range(3):
        start(step2[m, 0, k] for k in hops(PATHS[m][1]))
    for cp in ours + acopies:
        cp.wait()

    def pair(i, carry):
        at = (i // 8, pl.ds(pl.multiple_of(lax.rem(i, 8) * (rows // 8), 16), rows // 8))
        far = 1 - p.zl
        near_sum[at] = aown[(p.zl,) + at].astype(F32) + arecv[(p.zl,) + at].astype(F32)
        far_sum[at] = (aown[(far,) + at].astype(F32) + arecv[(far,) + at].astype(F32)).astype(BF16)
        return carry

    lax.fori_loop(0, 16, pair, 0)
    for i in (1, 3, 2):
        for m in range(3):
            if i in hops(PATHS[m][0]):
                step1[m, i].wait()
                start(step2[m, i, k] for k in hops(PATHS[m][1]))
    for group, relay, k in ((phase2a, relay_a, 1), (phase2b, relay_b, 3)):
        for cp in group:
            cp.wait()
        start(relay)
        start(swaps[k])
    for i in (0, 1, 3, 2):
        for m in range(3):
            if i < SIZE[PATHS[m][0]]:
                start(step3[m, i, 0, k] for k in hops(PATHS[m][2]))
                keep[m, i, 0].start()
    for i in (0, 1, 3, 2):
        for j in (1, 3, 2):
            for m in range(3):
                if i < SIZE[PATHS[m][0]] and j in hops(PATHS[m][1]):
                    step2[m, i, j].wait()
                    start(step3[m, i, j, k] for k in hops(PATHS[m][2]))
                    keep[m, i, j].start()
        if i == 1:
            for cp in relay_a + relay_b:
                cp.wait()
            start(swaps[2])
    for cp in sum(swaps, []) + list(keep.values()) + list(step3.values()):
        cp.wait()


def gather(w, tok, att):
    units = w.shape[2] // 32
    depth = w.shape[1]
    rows = att.shape[1] // 4
    dma = pltpu.SemaphoreType.DMA
    split = (3, 4, 4, 2, units, depth)
    return pl.pallas_call(
        gather_kernel,
        out_shape=(
            jax.ShapeDtypeStruct((3, units, depth * 32), BF16),
            jax.ShapeDtypeStruct((2, 4, 4, 4) + tok.shape, BF16),
            jax.ShapeDtypeStruct((2, rows, att.shape[2]), F32),
            jax.ShapeDtypeStruct((2, rows, att.shape[2]), BF16),
        ),
        in_specs=[pl.BlockSpec(memory_space=pl.ANY)] * 3,
        out_specs=[pl.BlockSpec(memory_space=pl.ANY)] * 2 + [pl.BlockSpec(memory_space=pltpu.VMEM)] * 2,
        scratch_shapes=[
            pltpu.VMEM(w.shape, BF16),
            pltpu.VMEM(split, BF16),
            pltpu.VMEM(split, BF16),
            pltpu.VMEM(split, BF16),
            pltpu.VMEM((w.shape[2], depth), F32),
            pltpu.VMEM(tok.shape, BF16),
            pltpu.VMEM((2, 2, rows, att.shape[2]), BF16),
            pltpu.VMEM((2, 2, rows, att.shape[2]), BF16),
            dma((9,)), dma((9,)), dma((24,)), dma((24,)), dma((64,)), dma((64,)),
            dma((33,)), dma((33,)), dma((12,)), dma((12,)), dma((2,)), dma((2,)), dma((48,)),
        ],
        compiler_params=pltpu.CompilerParams(
            collective_id=0, has_side_effects=True, vmem_limit_bytes=56 * 1024 * 1024
        ),
    )(w, tok, att)


def colour_lanes(width):
    tiles = width // 128
    cut = [0, -(-tiles // 3), -(-tiles // 3) + (tiles - tiles // 3) // 2, tiles]
    return [(cut[i] * 128, (cut[i + 1] - cut[i]) * 128) for i in range(3)]


def hidden_block(rows, weights):
    padded, width = weights.shape[1:]
    rows = rows.reshape(-1, rows.shape[-1])
    proj = lax.dot_general(
        rows[:, :width], weights[...].reshape(2 * padded, width), (((1,), (1,)), ((), ())),
        preferred_element_type=F32,
    )
    gate, up = proj[:, :padded], proj[:, padded:]
    extra = rows[:, width:].astype(F32)
    lane = lax.broadcasted_iota(jnp.int32, extra.shape, 1)
    expert = lax.axis_index("zl") * 2 + lax.axis_index("core")
    mine = (lane == expert) | (lane == expert + 4)
    weight = jnp.sum(jnp.where(mine, extra, 0.0), axis=1, keepdims=True)
    return (gate / (1.0 + jnp.exp(-gate)) * up * weight).astype(BF16)


def hidden_kernel(rows, ew, hid, copy, x, wv, down, held, sems):
    p = Place()
    units = ew.shape[1]
    first = p.shift("z", CHUNKS[0])
    spots = [wv.at[0, pl.ds(0, units)], wv.at[1, pl.ds(0, units)], down]
    xin = [pltpu.make_async_copy(rows.at[h, first], x.at[h], sems.at[6 + h]) for h in range(2)]
    loads = [pltpu.make_async_copy(ew.at[m], spots[m], sems.at[m]) for m in range(3)]
    stores = [pltpu.make_async_copy(spots[m], copy.at[m], sems.at[3 + m]) for m in range(3)]
    out = [pltpu.make_async_copy(held.at[h], hid.at[h], sems.at[8 + h]) for h in range(2)]
    for cp in (loads[0], loads[1], xin[0], xin[1], loads[2]):
        cp.start()
    xin[0].wait()
    for m in range(2):
        loads[m].wait()
        stores[m].start()
    for h in range(2):
        if h == 1:
            xin[1].wait()
            loads[2].wait()
            stores[2].start()
        held[h] = hidden_block(x[h], wv)[:, :units].reshape(held.shape[1:])
        out[h].start()
    for cp in stores + out:
        cp.wait()


def hidden_of(rows, ew):
    units, width = ew.shape[1:]
    padded = -(-units // 128) * 128
    shape = (2,) + rows.shape[2:5] + (units,)
    count = 2 * 16 * rows.shape[4]
    hbm = pl.BlockSpec(memory_space=pltpu.HBM)
    return pl.pallas_call(
        hidden_kernel,
        out_shape=(jax.ShapeDtypeStruct(shape, BF16), jax.ShapeDtypeStruct(ew.shape, BF16)),
        in_specs=[hbm] * 2,
        out_specs=[hbm] * 2,
        scratch_shapes=[
            pltpu.VMEM((2,) + rows.shape[2:], BF16),
            pltpu.VMEM((2, padded, width), BF16),
            pltpu.VMEM((units, width), BF16),
            pltpu.VMEM(shape, BF16),
            pltpu.SemaphoreType.DMA((10,)),
        ],
        compiler_params=pltpu.CompilerParams(vmem_limit_bytes=63 * 1024 * 1024),
        cost_estimate=pl.CostEstimate(
            flops=4 * count * units * width, bytes_accessed=4 * ew.size, transcendentals=count * units
        ),
    )(rows, ew)


CHUNKS = (1, 3, 2, 0)


def scatter_kernel(rows, hid_hbm, ew, out, x, wv, hid, down, snd, r0, s0, r1, s1, r2, s2, r3,
                   xs, xr, ss, rs, ls):
    p = Place()
    units = ew.shape[1]
    parts = [(h, j) for j in CHUNKS[1:] for h in (1, 0)]

    def fetch(n):
        h, j = parts[n]
        core = lax.rem(p.core + h, 2)
        return pltpu.make_async_copy(rows.at[core, p.shift("z", j)], x.at[n % 2], ls.at[4 + n])

    fetches = [fetch(n) for n in range(6)]
    loads = [
        pltpu.make_async_copy(ew.at[2], down, ls.at[0]),
        pltpu.make_async_copy(hid_hbm, hid.at[:, p.shift("z", CHUNKS[0])], ls.at[1]),
        pltpu.make_async_copy(ew.at[0], wv.at[0, pl.ds(0, units)], ls.at[2]),
        pltpu.make_async_copy(ew.at[1], wv.at[1, pl.ds(0, units)], ls.at[3]),
    ]
    for cp in loads + fetches[:2]:
        cp.start()
    bar = pltpu.get_barrier_semaphore()
    peers = [{"core": 1 - p.core}] + [p.along(a, k) for a in ("x", "y", "z") for k in (1, 2, 3)]
    for q in peers:
        pl.semaphore_signal(bar, inc=1, device_id=q, device_id_type=MESH)
    pl.semaphore_wait(bar, len(peers))
    loads[0].wait()
    loads[1].wait()
    cuts = colour_lanes(down.shape[1])

    def product(core, z, c):
        lo, n = cuts[c]
        rows = hid[core, z].reshape(-1, hid.shape[-1])
        value = jnp.dot(rows, down[:, lo:lo + n], preferred_element_type=F32)
        return value.reshape(4, 4, -1, n)

    def swap(j, c):
        z = p.shift("z", j)
        return pltpu.make_async_remote_copy(
            snd[c].at[z], r0[c].at[z], xs.at[j * 3 + c], xr.at[j * 3 + c],
            device_id={"core": 1 - p.core}, device_id_type=MESH,
        )

    swaps = {(j, c): swap(j, c) for j in range(4) for c in range(3)}
    number = iter(range(60))

    def remote(src, dst, axis, k):
        i = next(number)
        return pltpu.make_async_remote_copy(
            src, dst, ss.at[i], rs.at[i], device_id=p.along(axis, k), device_id_type=MESH
        )

    def give(j):
        z = p.shift("z", j)
        for c in range(3):
            snd[c][z] = product(1 - p.core, z, c).astype(BF16)
            swaps[j, c].start()

    stage1 = [[], [], []]

    def take(j):
        z = p.shift("z", j)
        for c, order in enumerate(ORDERS):
            value = product(p.core, z, c)
            swaps[j, c].wait()
            s0[c][z] = (value + r0[c][z].astype(F32)).astype(BF16)
            axis = order[0]
            if axis == "z":
                copies = [remote(s0[c].at[z], r1[c].at[j - 1], "z", j)] if j else []
            elif axis == "y":
                copies = [
                    remote(s0[c].at[z, p.shift("y", k)], r1[c].at[k - 1, z], "y", k) for k in (1, 3, 2)
                ]
            else:
                copies = [
                    remote(s0[c].at[z, :, p.shift("x", k)], r1[c].at[k - 1, z], "x", k) for k in (1, 3, 2)
                ]
            for cp in copies:
                cp.start()
            stage1[c] += copies

    def compute(n):
        h, j = parts[n]
        fetches[n].wait()
        value = hidden_block(x[n % 2], wv)[:, :units]
        hid[lax.rem(p.core + h, 2), p.shift("z", j)] = value.reshape(hid.shape[2:])
        if n + 2 < len(parts):
            fetches[n + 2].start()

    give(CHUNKS[0])
    loads[2].wait()
    loads[3].wait()
    compute(0)
    give(CHUNKS[1])
    take(CHUNKS[0])
    compute(1)
    compute(2)
    take(CHUNKS[1])
    give(CHUNKS[2])
    compute(3)
    compute(4)
    give(CHUNKS[3])
    take(CHUNKS[2])
    compute(5)
    take(CHUNKS[3])

    def pick(ref, left, axis, v):
        return ref.at[tuple(v if a == axis else slice(None) for a in left)]

    def left_after(order, phase):
        return [a for a in ("z", "y", "x") if a not in order[:phase]]

    def send(c, axis, src_of, dst):
        copies = [remote(src_of(p.shift(axis, k)), dst.at[k - 1], axis, k) for k in (1, 3, 2)]
        for cp in copies:
            cp.start()
        return copies

    stage2, stage3 = [], []
    for c, order in enumerate(ORDERS):
        for cp in stage1[c]:
            cp.wait()
        mine = pick(s0[c], left_after(order, 0), order[0], p.at[order[0]])

        def add(i, carry, c=c, mine=mine):
            at = (i // 4, lax.rem(i, 4))
            total = mine[at].astype(F32)
            for k in range(3):
                total += r1[c][(k,) + at].astype(F32)
            s1[c][at] = total.astype(BF16)
            return carry

        lax.fori_loop(0, 16, add, 0)
        left = left_after(order, 1)
        stage2.append(send(c, order[1], lambda v, c=c, left=left, a=order[1]: pick(s1[c], left, a, v), r2[c]))

    for c, order in enumerate(ORDERS):
        for cp in stage2[c]:
            cp.wait()
        mine = pick(s1[c], left_after(order, 1), order[1], p.at[order[1]])

        def add(i, carry, c=c, mine=mine):
            total = mine[i].astype(F32)
            for k in range(3):
                total += r2[c][k, i].astype(F32)
            s2[c][i] = total.astype(BF16)
            return carry

        lax.fori_loop(0, 4, add, 0)
        left = left_after(order, 2)
        stage3.append(send(c, order[2], lambda v, c=c, left=left, a=order[2]: pick(s2[c], left, a, v), r3[c]))

    for c, order in enumerate(ORDERS):
        for cp in stage3[c]:
            cp.wait()
        total = s2[c][p.at[order[2]]].astype(F32)
        for k in range(3):
            total += r3[c][k].astype(F32)
        lo, n = cuts[c]
        out[:, lo:lo + n] = total.astype(BF16)


def scatter(tall, hid, ew):
    rows, units = hid.shape[-2:]
    width = ew.shape[2]
    padded = -(-units // 128) * 128
    cuts = colour_lanes(width)
    dma = pltpu.SemaphoreType.DMA

    def bufs(*lead):
        return [pltpu.VMEM(lead + (rows, n), BF16) for _, n in cuts]

    return pl.pallas_call(
        scatter_kernel,
        out_shape=jax.ShapeDtypeStruct((rows, width), BF16),
        in_specs=[pl.BlockSpec(memory_space=pltpu.HBM)] * 3,
        out_specs=pl.BlockSpec(memory_space=pltpu.VMEM),
        scratch_shapes=[
            pltpu.VMEM((2,) + tall.shape[2:], BF16),
            pltpu.VMEM((2, padded, width), BF16),
            pltpu.VMEM((2, 4, 4, 4, rows, units), BF16),
            pltpu.VMEM((units, width), BF16),
            bufs(4, 4, 4), bufs(4, 4, 4), bufs(4, 4, 4),
            bufs(3, 4, 4), bufs(4, 4), bufs(3, 4), bufs(4), bufs(3),
            dma((12,)), dma((12,)), dma((60,)), dma((60,)), dma((10,)),
        ],
        compiler_params=pltpu.CompilerParams(
            collective_id=1, has_side_effects=True, vmem_limit_bytes=60 * 1024 * 1024
        ),
    )(tall, hid, ew)


def local(attention_weights, ffn_weights, tokens, routes, router):
    experts = router.shape[1]
    width = tokens.shape[1]
    gates = jax.nn.sigmoid(jnp.dot(tokens, router, preferred_element_type=F32))
    named = jnp.sum((routes[:, :, None] == jnp.arange(experts, dtype=jnp.int32)).astype(F32), axis=1)
    weighting = named * gates
    high = lax.reduce_precision(weighting, 8, 7)
    low = (weighting - high).astype(BF16)
    high = high.astype(BF16)
    tok = jnp.concatenate(
        [tokens, high, low, jnp.zeros((tokens.shape[0], 128 - 2 * experts), BF16)], axis=1
    )
    ew, tall, near_sum, far_sum = gather(ffn_weights[0], tok, attention_weights[0])
    hid, kept = hidden_of(tall, ew)
    mixed_output = scatter(tall, hid, kept)
    far = lax.ppermute(far_sum, "zl", [(0, 1), (1, 0)])
    merged = ((near_sum + far.astype(F32)) * 0.25).astype(BF16)
    return merged, jnp.swapaxes(kept, 1, 2)[None], mixed_output


def solution(mesh):
    torus = Mesh(mesh.devices.reshape(2, 2, 4, 4, 2), ("zl", "core", "y", "x", "zh"))
    shard = ("y", "x", "zh")
    branch = ("zl", "core")
    in_specs = (
        P(branch, None, None, shard),
        P(branch, None, shard, None),
        P(branch + shard, None),
        P(branch + shard, None),
        P(),
    )
    out_specs = (P(None, branch, shard), P(branch, None, None, shard), P(branch + shard, None))
    return jax.shard_map(local, mesh=torus, in_specs=in_specs, out_specs=out_specs, check_vma=False)
```

```python
import jax
import jax.numpy as jnp
from jax import lax
from jax.experimental import pallas as pl
from jax.experimental.pallas import tpu as pltpu
from jax.sharding import Mesh
from jax.sharding import PartitionSpec as P

MESH = pl.DeviceIdType.MESH
BF16 = jnp.bfloat16
F32 = jnp.float32

PATHS = (("zh", "x", "y"), ("y", "zh", "x"), ("x", "y", "zh"))
SIZE = {"y": 4, "x": 4, "zh": 2}
GRID = ("y", "x", "zh")
ORDERS = (("x", "y", "z"), ("y", "z", "x"), ("z", "x", "y"))


class Place:
    def __init__(self):
        self.y, self.x = lax.axis_index("y"), lax.axis_index("x")
        self.zh, self.zl = lax.axis_index("zh"), lax.axis_index("zl")
        self.core = lax.axis_index("core")
        self.z = self.zh * 2 + self.zl
        self.at = {"x": self.x, "y": self.y, "z": self.z}

    def shift(self, axis, k):
        return lax.rem(self.at[axis] + k, 4)

    def along(self, axis, k):
        v = self.shift(axis, k)
        if axis == "z":
            return {"zh": v // 2, "zl": lax.rem(v, 2)}
        return {axis: v}

    def shard(self, o):
        return lax.rem(self.y + o[0], 4), lax.rem(self.x + o[1], 4), lax.rem(self.zh + o[2], 2)


def block_index(place, order, phase, coords=None):
    done = order[:phase]
    out = []
    for axis in ("z", "y", "x"):
        if axis in done:
            out.append(slice(None))
        else:
            out.append(place.at[axis] if coords is None or axis not in coords else coords[axis])
    return tuple(out)


def gather_kernel(w, tok, ext, att, ew, tall, near_sum, far_sum, raw, wt, b1, b2, turned, tbuf, aown, arecv,
                  s1, r1, s2, r2, s3, r3, gs, gr, cs, cr, as_, ar, ls):
    p = Place()
    rows = att.shape[1] // 4
    width = tok.shape[1]
    third = tall.shape[-1] // 3
    units = ew.shape[1]
    pos = {"y": p.y, "x": p.x, "zh": p.zh}

    def near(axis, k):
        return lax.rem(pos[axis] + k, SIZE[axis])

    def start(copies):
        for cp in copies:
            cp.start()

    loads = [pltpu.make_async_copy(w.at[m], raw.at[m], ls.at[m]) for m in range(3)]
    tins = [
        pltpu.make_async_copy(tok, tbuf.at[:, pl.ds(0, width)], ls.at[3]),
        pltpu.make_async_copy(ext, tbuf.at[:, pl.ds(width, ext.shape[1])], ls.at[47]),
    ]
    tout = pltpu.make_async_copy(tbuf, tall.at[p.core, p.z, p.y, p.x], ls.at[4])
    start(tins)
    start(loads)
    ours = [
        pltpu.make_async_copy(
            att.at[:, pl.ds(pl.multiple_of((z * 2 + p.core) * rows, 8), rows), :], aown.at[z], ls.at[45 + z]
        )
        for z in range(2)
    ]
    start(ours)

    bar = pltpu.get_barrier_semaphore()
    peers = [p.along(a, k) for a in ("x", "y", "z") for k in (1, 2, 3)]
    peers += [{"core": 1 - p.core}]
    for q in peers:
        pl.semaphore_signal(bar, inc=1, device_id=q, device_id_type=MESH)
    pl.semaphore_wait(bar, len(peers))

    def lanes(c):
        return pl.ds(c * third, third)

    def gather_copies(phase, hops_):
        out = []
        for c, order in enumerate(ORDERS):
            at = (p.core,) + block_index(p, order, phase) + (slice(None),)
            dst = tall.at[at + (lanes(c),)]
            pairs = [(dst, dst, (phase * 3 + c) * 3)]
            if phase == 0:
                end = min((c + 1) * third, width)
                cut = pl.ds(c * third, end - c * third)
                pairs = [(tok.at[:, cut], tall.at[at + (cut,)], c * 3)]
                if c == 2:
                    pairs.append((ext, tall.at[at + (pl.ds(width, ext.shape[1]),)], 33))
            for src, dst, first in pairs:
                for k in hops_:
                    i = first + k - 1
                    out.append(
                        pltpu.make_async_remote_copy(
                            src, dst, gs.at[i], gr.at[i],
                            device_id=p.along(order[phase], k), device_id_type=MESH,
                        )
                    )
        return out

    def relay_copies(back):
        out = []
        for c, order in enumerate(ORDERS):
            axis = order[2]
            at = list(block_index(p, order, 2, {axis: p.shift(axis, 4 - back)}))
            split = [n for n in range(3) if isinstance(at[n], slice)][0]
            at[split] = pl.ds(0 if back == 1 else 2, 2)
            ref = tall.at[(p.core,) + tuple(at) + (slice(None), lanes(c))]
            i = 27 + c * 2 + (0 if back == 1 else 1)
            out.append(
                pltpu.make_async_remote_copy(
                    ref, ref, gs.at[i], gr.at[i],
                    device_id=p.along(axis, back), device_id_type=MESH,
                )
            )
        return out

    def blocks(ref, **fixed):
        return ref.at[tuple(fixed.get(a, slice(None)) for a in GRID)]

    def remote(src, dst, send, recv, axis, k):
        return pltpu.make_async_remote_copy(
            src, dst, send, recv, device_id={axis: near(axis, k)}, device_id_type=MESH
        )

    def hops(axis):
        return (1, 3, 2) if SIZE[axis] == 4 else (1,)

    def column(ref, m, y, x, zh):
        lane = ((y * 4 + x) * 2 + zh) * 128
        return ref.at[m, :, pl.ds(pl.multiple_of(lane, 128), 128)]

    step1, step2, step3, keep = {}, {}, {}, {}
    number2 = number3 = 0
    for m, (a, b, c) in enumerate(PATHS):
        for k in hops(a):
            step1[m, k] = remote(
                blocks(wt.at[m], **{a: near(a, k)}), blocks(b1.at[m], **{a: pos[a]}),
                s1.at[m * 3 + k - 1], r1.at[m * 3 + k - 1], a, k,
            )
        for i in range(SIZE[a]):
            src_a = near(a, SIZE[a] - i)
            first = wt if i == 0 else b1
            for k in hops(b):
                step2[m, i, k] = remote(
                    blocks(first.at[m], **{a: src_a, b: near(b, k)}),
                    blocks(b2.at[m], **{a: src_a, b: pos[b]}),
                    s2.at[number2], r2.at[number2], b, k,
                )
                number2 += 1
            for j in range(SIZE[b]):
                src_b = near(b, SIZE[b] - j)
                held = first if j == 0 else b2
                for k in hops(c):
                    step3[m, i, j, k] = remote(
                        blocks(held.at[m], **{a: src_a, b: src_b, c: near(c, k)}),
                        column(ew, m, **{a: src_a, b: src_b, c: pos[c]}),
                        s3.at[number3], r3.at[number3], c, k,
                    )
                    number3 += 1
                keep[m, i, j] = pltpu.make_async_copy(
                    blocks(held.at[m], **{a: src_a, b: src_b, c: pos[c]}),
                    column(ew, m, **{a: src_a, b: src_b, c: pos[c]}),
                    ls.at[5 + len(keep)],
                )

    phase0, phase1 = gather_copies(0, (1, 3, 2)), gather_copies(1, (1, 3, 2))
    phase2a, phase2b = gather_copies(2, (1,)), gather_copies(2, (3,))
    relay_a, relay_b = relay_copies(1), relay_copies(3)
    def swap_copies(k):
        out = []
        for c, order in enumerate(ORDERS):
            at = block_index(p, order, 2, {order[2]: p.shift(order[2], 4 - k)})
            ref = tall.at[(p.core,) + at + (slice(None), lanes(c))]
            out.append(
                pltpu.make_async_remote_copy(
                    ref, ref, cs.at[c * 4 + k], cr.at[c * 4 + k],
                    device_id={"core": 1 - p.core}, device_id_type=MESH,
                )
            )
        return out

    swaps = [swap_copies(k) for k in range(4)]
    acopies = [
        pltpu.make_async_remote_copy(
            att.at[:, pl.ds(pl.multiple_of((z * 2 + 1 - p.core) * rows, 8), rows), :],
            arecv.at[z], as_.at[z], ar.at[z],
            device_id={"core": 1 - p.core}, device_id_type=MESH,
        )
        for z in range(2)
    ]

    start(phase0)
    start(acopies)
    for cp in tins:
        cp.wait()
    tout.start()
    tout.wait()

    def turn(m):
        def body(i, carry):
            at = pl.ds(pl.multiple_of(i * 256, 256), 256)
            turned[at, :] = raw[m, :, at].T.astype(F32)
            return carry

        def place(d, carry):
            piece = turned[pl.ds(pl.multiple_of(d * units, 8), units), :]
            wt[m, d // 8, lax.rem(d // 2, 4), lax.rem(d, 2)] = piece.astype(BF16)
            return carry

        lax.fori_loop(0, raw.shape[2] // 256, body, 0, unroll=2)
        lax.fori_loop(0, 32, place, 0, unroll=4)

    for m in range(3):
        loads[m].wait()
        turn(m)
        start(step1[m, k] for k in hops(PATHS[m][0]))
        if m == 0:
            for cp in phase0:
                cp.wait()
            start(phase1)
        if m == 2:
            for cp in phase1:
                cp.wait()
            start(phase2a)
            start(phase2b)
            start(swaps[0])
    for m in range(3):
        start(step2[m, 0, k] for k in hops(PATHS[m][1]))
    for cp in ours + acopies:
        cp.wait()

    def pair(i, carry):
        at = (i // 8, pl.ds(pl.multiple_of(lax.rem(i, 8) * (rows // 8), 16), rows // 8))
        far = 1 - p.zl
        near_sum[at] = aown[(p.zl,) + at].astype(F32) + arecv[(p.zl,) + at].astype(F32)
        far_sum[at] = (aown[(far,) + at].astype(F32) + arecv[(far,) + at].astype(F32)).astype(BF16)
        return carry

    lax.fori_loop(0, 16, pair, 0)
    for i in (1, 3, 2):
        for m in range(3):
            if i in hops(PATHS[m][0]):
                step1[m, i].wait()
                start(step2[m, i, k] for k in hops(PATHS[m][1]))
    for group, relay, k in ((phase2a, relay_a, 1), (phase2b, relay_b, 3)):
        for cp in group:
            cp.wait()
        start(relay)
        start(swaps[k])
    for i in (0, 1, 3, 2):
        for m in range(3):
            if i < SIZE[PATHS[m][0]]:
                start(step3[m, i, 0, k] for k in hops(PATHS[m][2]))
                keep[m, i, 0].start()
    for i in (0, 1, 3, 2):
        for j in (1, 3, 2):
            for m in range(3):
                if i < SIZE[PATHS[m][0]] and j in hops(PATHS[m][1]):
                    step2[m, i, j].wait()
                    start(step3[m, i, j, k] for k in hops(PATHS[m][2]))
                    keep[m, i, j].start()
        if i == 1:
            for cp in relay_a + relay_b:
                cp.wait()
            start(swaps[2])
    for cp in sum(swaps, []) + list(keep.values()) + list(step3.values()):
        cp.wait()


def gather(w, tok, ext, att):
    units = w.shape[2] // 32
    depth = w.shape[1]
    rows = att.shape[1] // 4
    dma = pltpu.SemaphoreType.DMA
    split = (3, 4, 4, 2, units, depth)
    wide = (tok.shape[0], tok.shape[1] + ext.shape[1])
    return pl.pallas_call(
        gather_kernel,
        out_shape=(
            jax.ShapeDtypeStruct((3, units, depth * 32), BF16),
            jax.ShapeDtypeStruct((2, 4, 4, 4) + wide, BF16),
            jax.ShapeDtypeStruct((2, rows, att.shape[2]), F32),
            jax.ShapeDtypeStruct((2, rows, att.shape[2]), BF16),
        ),
        in_specs=[pl.BlockSpec(memory_space=pltpu.HBM)] * 4,
        out_specs=[pl.BlockSpec(memory_space=pl.ANY)] * 2 + [pl.BlockSpec(memory_space=pltpu.VMEM)] * 2,
        scratch_shapes=[
            pltpu.VMEM(w.shape, BF16),
            pltpu.VMEM(split, BF16),
            pltpu.VMEM(split, BF16),
            pltpu.VMEM(split, BF16),
            pltpu.VMEM((w.shape[2], depth), F32),
            pltpu.VMEM(wide, BF16),
            pltpu.VMEM((2, 2, rows, att.shape[2]), BF16),
            pltpu.VMEM((2, 2, rows, att.shape[2]), BF16),
            dma((9,)), dma((9,)), dma((24,)), dma((24,)), dma((64,)), dma((64,)),
            dma((36,)), dma((36,)), dma((12,)), dma((12,)), dma((2,)), dma((2,)), dma((48,)),
        ],
        compiler_params=pltpu.CompilerParams(
            collective_id=0, has_side_effects=True, vmem_limit_bytes=56 * 1024 * 1024
        ),
    )(w, tok, ext, att)


def colour_lanes(width):
    tiles = width // 128
    cut = [0, -(-tiles // 3), -(-tiles // 3) + (tiles - tiles // 3) // 2, tiles]
    return [(cut[i] * 128, (cut[i + 1] - cut[i]) * 128) for i in range(3)]


def hidden_block(rows, weights):
    padded, width = weights.shape[1:]
    rows = rows.reshape(-1, rows.shape[-1])
    proj = lax.dot_general(
        rows[:, :width], weights[...].reshape(2 * padded, width), (((1,), (1,)), ((), ())),
        preferred_element_type=F32,
    )
    gate, up = proj[:, :padded], proj[:, padded:]
    extra = rows[:, width:].astype(F32)
    lane = lax.broadcasted_iota(jnp.int32, extra.shape, 1)
    expert = lax.axis_index("zl") * 2 + lax.axis_index("core")
    mine = (lane == expert) | (lane == expert + 4)
    weight = jnp.sum(jnp.where(mine, extra, 0.0), axis=1, keepdims=True)
    return (gate / (1.0 + jnp.exp(-gate)) * up * weight).astype(BF16)


def hidden_kernel(rows, ew, hid, copy, x, wv, down, held, sems):
    p = Place()
    units = ew.shape[1]
    first = p.shift("z", CHUNKS[0])
    spots = [wv.at[0, pl.ds(0, units)], wv.at[1, pl.ds(0, units)], down]
    xin = [pltpu.make_async_copy(rows.at[h, first], x.at[h], sems.at[6 + h]) for h in range(2)]
    loads = [pltpu.make_async_copy(ew.at[m], spots[m], sems.at[m]) for m in range(3)]
    stores = [pltpu.make_async_copy(spots[m], copy.at[m], sems.at[3 + m]) for m in range(3)]
    out = [pltpu.make_async_copy(held.at[h], hid.at[h], sems.at[8 + h]) for h in range(2)]
    for cp in (loads[0], loads[1], xin[0], xin[1], loads[2]):
        cp.start()
    xin[0].wait()
    for m in range(2):
        loads[m].wait()
        stores[m].start()
    for h in range(2):
        if h == 1:
            xin[1].wait()
            loads[2].wait()
            stores[2].start()
        held[h] = hidden_block(x[h], wv)[:, :units].reshape(held.shape[1:])
        out[h].start()
    for cp in stores + out:
        cp.wait()


def hidden_of(rows, ew):
    units, width = ew.shape[1:]
    padded = -(-units // 128) * 128
    shape = (2,) + rows.shape[2:5] + (units,)
    count = 2 * 16 * rows.shape[4]
    hbm = pl.BlockSpec(memory_space=pltpu.HBM)
    return pl.pallas_call(
        hidden_kernel,
        out_shape=(jax.ShapeDtypeStruct(shape, BF16), jax.ShapeDtypeStruct(ew.shape, BF16)),
        in_specs=[hbm] * 2,
        out_specs=[hbm] * 2,
        scratch_shapes=[
            pltpu.VMEM((2,) + rows.shape[2:], BF16),
            pltpu.VMEM((2, padded, width), BF16),
            pltpu.VMEM((units, width), BF16),
            pltpu.VMEM(shape, BF16),
            pltpu.SemaphoreType.DMA((10,)),
        ],
        compiler_params=pltpu.CompilerParams(vmem_limit_bytes=63 * 1024 * 1024),
        cost_estimate=pl.CostEstimate(
            flops=4 * count * units * width, bytes_accessed=4 * ew.size, transcendentals=count * units
        ),
    )(rows, ew)


CHUNKS = (2, 1, 3, 0)


def scatter_kernel(rows, hid_hbm, ew, out, x, wv, hid, down, snd, r0, s0, e1, r1, s1, r2, s2, r3,
                   xs, xr, ss, rs, ls):
    p = Place()
    units = ew.shape[1]
    parts = [(h, j) for j in CHUNKS[1:] for h in (1, 0)]

    def fetch(n):
        h, j = parts[n]
        core = lax.rem(p.core + h, 2)
        return pltpu.make_async_copy(rows.at[core, p.shift("z", j)], x.at[n % 2], ls.at[4 + n])

    fetches = [fetch(n) for n in range(6)]
    loads = [
        pltpu.make_async_copy(ew.at[2], down, ls.at[0]),
        pltpu.make_async_copy(hid_hbm, hid.at[:, p.shift("z", CHUNKS[0])], ls.at[1]),
        pltpu.make_async_copy(ew.at[0], wv.at[0, pl.ds(0, units)], ls.at[2]),
        pltpu.make_async_copy(ew.at[1], wv.at[1, pl.ds(0, units)], ls.at[3]),
    ]
    loads[0].start()
    loads[1].start()
    bar = pltpu.get_barrier_semaphore()
    peers = [{"core": 1 - p.core}] + [p.along(a, k) for a in ("x", "y", "z") for k in (1, 2, 3)]
    for q in peers:
        pl.semaphore_signal(bar, inc=1, device_id=q, device_id_type=MESH)
    pl.semaphore_wait(bar, len(peers))
    loads[0].wait()
    loads[1].wait()
    for cp in loads[2:] + fetches[:2]:
        cp.start()
    cuts = colour_lanes(down.shape[1])

    def product(core, z, c):
        lo, n = cuts[c]
        rows = hid[core, z].reshape(-1, hid.shape[-1])
        value = jnp.dot(rows, down[:, lo:lo + n], preferred_element_type=F32)
        return value.reshape(4, 4, -1, n)

    def swap(j, c):
        z = p.shift("z", j)
        return pltpu.make_async_remote_copy(
            snd[c].at[z], r0[c].at[z], xs.at[j * 3 + c], xr.at[j * 3 + c],
            device_id={"core": 1 - p.core}, device_id_type=MESH,
        )

    swaps = {(j, c): swap(j, c) for j in range(4) for c in range(3)}
    number = iter(range(63))

    def remote(src, dst, axis, k):
        i = next(number)
        return pltpu.make_async_remote_copy(
            src, dst, ss.at[i], rs.at[i], device_id=p.along(axis, k), device_id_type=MESH
        )

    def give(j):
        z = p.shift("z", j)
        for c in range(3):
            snd[c][z] = product(1 - p.core, z, c).astype(BF16)
            swaps[j, c].start()

    early, stage1 = {}, {}
    halves = (pl.ds(0, 2), pl.ds(2, 2))

    def begin(copies):
        for cp in copies:
            cp.start()
        return copies

    def slab(c, z, v, part=slice(None)):
        return s0[c].at[z, part, v] if c == 0 else s0[c].at[z, v, part]

    def take(j):
        z = p.shift("z", j)
        for c, order in enumerate(ORDERS):
            value = product(p.core, z, c)
            swaps[j, c].wait()
            s0[c][z] = (value + r0[c][z].astype(F32)).astype(BF16)
            axis = order[0]
            if axis != "z":
                far = p.shift(axis, 2)
                early[c, j] = begin([
                    remote(slab(c, z, far, halves[i]), e1[c].at[i, z], axis, k) for i, k in ((0, 1), (1, 3))
                ])
            elif j == 2:
                early[c] = begin([
                    remote(s0[c].at[z, halves[i]], e1[c].at[i], axis, k) for i, k in ((0, 1), (1, 3))
                ])
            elif j:
                i = 0 if j == 1 else 1
                early[c][i].wait()

                def join(n, carry, c=c, i=i):
                    at = (z, i * 2 + n // 4, lax.rem(n, 4))
                    term = e1[c][i, n // 4, lax.rem(n, 4)].astype(F32)
                    s0[c][at] = (s0[c][at].astype(F32) + term).astype(BF16)
                    return carry

                lax.fori_loop(0, 8, join, 0)
                stage1[c, j] = begin([remote(s0[c].at[z], r1[c].at[i], axis, j)])

    def relay(j):
        z = p.shift("z", j)
        for c in (0, 1):
            axis = ORDERS[c][0]
            for cp in early[c, j]:
                cp.wait()
            stage1[c, j] = []
            for i, k in ((0, 1), (1, 3)):
                v = p.shift(axis, k)

                def join(n, carry, c=c, i=i, v=v):
                    at = (z, i * 2 + n, v) if c == 0 else (z, v, i * 2 + n)
                    s0[c][at] = (s0[c][at].astype(F32) + e1[c][i, z, n].astype(F32)).astype(BF16)
                    return carry

                lax.fori_loop(0, 2, join, 0)
                stage1[c, j] += begin([remote(slab(c, z, v), r1[c].at[i, z], axis, k)])

    def compute(n):
        h, j = parts[n]
        fetches[n].wait()
        value = hidden_block(x[n % 2], wv)[:, :units]
        hid[lax.rem(p.core + h, 2), p.shift("z", j)] = value.reshape(hid.shape[2:])
        if n + 2 < len(parts):
            fetches[n + 2].start()

    stage2, stage3 = {}, []

    def reduce(j):
        z = p.shift("z", j)
        for c in (0, 1):
            for cp in stage1[c, j]:
                cp.wait()

            def add(i, carry, c=c):
                mine = s0[c][z, i, p.x] if c == 0 else s0[c][z, p.y, i]
                total = mine.astype(F32)
                for k in range(2):
                    total += r1[c][k, z, i].astype(F32)
                s1[c][z, i] = total.astype(BF16)
                return carry

            lax.fori_loop(0, 4, add, 0)
            if c == 0:
                copies = [
                    remote(s1[c].at[z, p.shift("y", k)], r2[c].at[k - 1, z], "y", k) for k in (1, 3, 2)
                ]
            else:
                copies = [remote(s1[c].at[z], r2[c].at[j - 1], "z", j)] if j else []
            for cp in copies:
                cp.start()
            stage2[c] = stage2.get(c, []) + copies

    give(2)
    loads[2].wait()
    loads[3].wait()
    compute(0)
    give(1)
    take(2)
    compute(1)
    compute(2)
    take(1)
    relay(2)
    give(3)
    compute(3)
    relay(1)
    take(3)
    compute(4)
    give(0)
    relay(3)
    reduce(2)
    compute(5)
    take(0)
    reduce(1)
    relay(0)
    reduce(3)

    def pick(ref, left, axis, v):
        return ref.at[tuple(v if a == axis else slice(None) for a in left)]

    def left_after(order, phase):
        return [a for a in ("z", "y", "x") if a not in order[:phase]]

    def send(c, axis, src_of, dst):
        copies = [remote(src_of(p.shift(axis, k)), dst.at[k - 1], axis, k) for k in (1, 3, 2)]
        for cp in copies:
            cp.start()
        return copies

    for j in (1, 3):
        stage1[2, j][0].wait()
    own = p.z

    def add(i, carry):
        at = (i // 4, lax.rem(i, 4))
        total = s0[2][(own,) + at].astype(F32)
        for k in range(2):
            total += r1[2][(k,) + at].astype(F32)
        s1[2][at] = total.astype(BF16)
        return carry

    lax.fori_loop(0, 16, add, 0)
    stage2[2] = send(2, "x", lambda v: s1[2].at[:, v], r2[2])
    reduce(0)

    for c, order in enumerate(ORDERS):
        for cp in stage2[c]:
            cp.wait()
        mine = pick(s1[c], left_after(order, 1), order[1], p.at[order[1]])

        def add(i, carry, c=c, mine=mine):
            total = mine[i].astype(F32)
            for k in range(3):
                total += r2[c][k, i].astype(F32)
            s2[c][i] = total.astype(BF16)
            return carry

        lax.fori_loop(0, 4, add, 0)
        left = left_after(order, 2)
        stage3.append(send(c, order[2], lambda v, c=c, left=left, a=order[2]: pick(s2[c], left, a, v), r3[c]))

    for c, order in enumerate(ORDERS):
        for cp in stage3[c]:
            cp.wait()
        total = s2[c][p.at[order[2]]].astype(F32)
        for k in range(3):
            total += r3[c][k].astype(F32)
        lo, n = cuts[c]
        out[:, lo:lo + n] = total.astype(BF16)


def scatter(tall, hid, ew):
    rows, units = hid.shape[-2:]
    width = ew.shape[2]
    padded = -(-units // 128) * 128
    cuts = colour_lanes(width)
    dma = pltpu.SemaphoreType.DMA

    def bufs(*lead):
        return [pltpu.VMEM(lead + (rows, n), BF16) for _, n in cuts]

    return pl.pallas_call(
        scatter_kernel,
        out_shape=jax.ShapeDtypeStruct((rows, width), BF16),
        in_specs=[pl.BlockSpec(memory_space=pltpu.HBM)] * 3,
        out_specs=pl.BlockSpec(memory_space=pltpu.VMEM),
        scratch_shapes=[
            pltpu.VMEM((2,) + tall.shape[2:], BF16),
            pltpu.VMEM((2, padded, width), BF16),
            pltpu.VMEM((2, 4, 4, 4, rows, units), BF16),
            pltpu.VMEM((units, width), BF16),
            bufs(4, 4, 4), bufs(4, 4, 4), bufs(4, 4, 4),
            [pltpu.VMEM(lead + (rows, n), BF16)
             for lead, (_, n) in zip(((2, 4, 2), (2, 4, 2), (2, 2, 4)), cuts)],
            bufs(2, 4, 4), bufs(4, 4), bufs(3, 4), bufs(4), bufs(3),
            dma((12,)), dma((12,)), dma((63,)), dma((63,)), dma((10,)),
        ],
        compiler_params=pltpu.CompilerParams(
            collective_id=1, has_side_effects=True, vmem_limit_bytes=60 * 1024 * 1024
        ),
    )(tall, hid, ew)


def local(attention_weights, ffn_weights, tokens, routes, router):
    experts = router.shape[1]
    width = tokens.shape[1]
    gates = jax.nn.sigmoid(jnp.dot(tokens, router, preferred_element_type=F32))
    named = jnp.sum((routes[:, :, None] == jnp.arange(experts, dtype=jnp.int32)).astype(F32), axis=1)
    weighting = named * gates
    high = lax.reduce_precision(weighting, 8, 7)
    low = (weighting - high).astype(BF16)
    high = high.astype(BF16)
    ext = jnp.concatenate(
        [high, low, jnp.zeros((tokens.shape[0], 128 - 2 * experts), BF16)], axis=1
    )
    ew, tall, near_sum, far_sum = gather(ffn_weights[0], tokens, ext, attention_weights[0])
    hid, kept = hidden_of(tall, ew)
    mixed_output = scatter(tall, hid, kept)
    far = lax.ppermute(far_sum, "zl", [(0, 1), (1, 0)])
    merged = ((near_sum + far.astype(F32)) * 0.25).astype(BF16)
    return merged, jnp.swapaxes(kept, 1, 2)[None], mixed_output


def solution(mesh):
    torus = Mesh(mesh.devices.reshape(2, 2, 4, 4, 2), ("zl", "core", "y", "x", "zh"))
    shard = ("y", "x", "zh")
    branch = ("zl", "core")
    in_specs = (
        P(branch, None, None, shard),
        P(branch, None, shard, None),
        P(branch + shard, None),
        P(branch + shard, None),
        P(),
    )
    out_specs = (P(None, branch, shard), P(branch, None, None, shard), P(branch + shard, None))
    return jax.shard_map(local, mesh=torus, in_specs=in_specs, out_specs=out_specs, check_vma=False)
```
